128 devices in a mesh: row: 8 (over y_hi, z), col: 16 (over x, y_lo, core).
Axes of the slice: x: 4, y: 4 (y_hi: 2, y_lo: 2; y = y_hi * 2 + y_lo), z: 4, core: 2. Of those that a mesh axis runs over, the one named last changes fastest.
Arguments:
- grad: float32 [8192, 14336], P(('row', 'col')), may hold values from -30 to 30
- momentum: float32 [8192, 14336], P(('row', 'col')), may hold values from -6 to 6
- weight: float32 [8192, 14336], P(('row', 'col')), may hold values from -0.75 to 0.75
Outputs:
- new_weight: float32 [8192, 14336], P('row', 'col')
- new_momentum: float32 [8192, 14336], P('row', 'col')
The draws below stay inside these ranges and needn't reach their ends.
All inputs are finite; a program needn't handle non-finite values.
Results may differ from the reference program's by a relative error of at most 0.00002.
Values sent between devices are 32-bit elements; how exact they have to be, the bound alone decides.
A program may use at most 128 MiB of HBM per device.

```python
import math
import jax
import jax.numpy as jnp

D = 8192
FF = 14336


def draw_grad(key, part):
    key_rows, key_cols, key_base = jax.random.split(key, 3)
    row_scale = jnp.exp(jax.random.uniform(key_rows, (D, 1), jnp.float32) * jnp.log(10.0))
    col_scale = jnp.exp(jax.random.uniform(key_cols, (1, FF), jnp.float32) * jnp.log(10.0))
    ramp = 1.0 + 2.0 * jnp.arange(D, dtype=jnp.float32).reshape(D, 1) / (D - 1)
    base = jnp.clip(jax.random.normal(key_base, (D, FF), jnp.float32), -6.0, 6.0)
    scaled = base * row_scale * col_scale * ramp / 10.0
    return jnp.clip(scaled, -30.0, 30.0).astype(jnp.float32)


def levels(stream_key, extent, shards, low, high):
    level, own = 1.0, jax.random.fold_in(stream_key, 6)
    for position, shards_of in shards:
        draws = jnp.exp(jax.random.uniform(jax.random.fold_in(own, position), (shards_of,), jnp.float32, low / len(shards), high / len(shards)))
        level = level * jnp.repeat(draws, extent[position] // shards_of).reshape([-1 if axis == position else 1 for axis in range(len(extent))])
    return level


def gaussian(rng, shape, deviation, bound, shards=(), held_as=jnp.bfloat16):
    loudness = levels(rng, shape, shards, -0.22, 0.18) if shards else 1.0
    drawn = jax.random.normal(rng, shape, jnp.float32) * deviation * loudness
    return jnp.minimum(jnp.maximum(drawn, -bound), bound).astype(held_as)


def setup_inputs(seed: int = 0) -> dict:
    seeds = jax.random.split(jax.random.key(seed), 4)
    return {
        "grad": draw_grad(jax.random.fold_in(seeds[3], 71), 0),
        "momentum": gaussian(seeds[1], (D, FF), 1.0, 6.0, ((0, 128),), jnp.float32),
        "weight": gaussian(seeds[2], (D, FF), 0.05, 0.75, ((0, 128),), jnp.float32),
    }


def reference(grad, momentum, weight):
    total = jnp.sum(grad * grad)
    limit = jnp.float32(math.sqrt(D * FF))
    factor = jnp.minimum(jnp.float32(1.0), limit / (jnp.sqrt(total) + jnp.float32(1e-06)))
    new_momentum = jnp.float32(0.9) * momentum + factor * grad
    new_weight = weight - jnp.float32(0.1) * new_momentum
    return (new_weight, new_momentum)
```

```python
import math

import jax
import jax.numpy as jnp
from jax import lax
from jax.experimental import pallas as pl
from jax.experimental.pallas import tpu as pltpu
from jax.sharding import PartitionSpec as P

D = 8192
FF = 14336
MESH = pl.DeviceIdType.MESH
LIMIT = math.sqrt(D * FF)

NX, NY, NC = 4, 2, 2
PEERS = NX * NY * NC
ROWS, COLS = 64, 896
ZS = 4

STEPS = sorted(
    [(a, b, c) for a in range(NX) for b in range(NY) for c in range(NC) if a or b or c],
    key=lambda s: -min(s[0], NX - s[0]) - s[1],
)
PLANE = [(a, h, b, c) for a in range(NX) for h in range(2) for b in range(NY) for c in range(NC)][1:]


def kernel(g_hbm, m_hbm, w_hbm, nw, nm, g, m, w, out, part, plane, line, load, w_send, w_recv, m_send, m_recv, p_send, p_recv, z_send, z_recv):
    col, row = lax.axis_index("col"), lax.axis_index("row")
    x, y, c = col // (NY * NC), (col // NC) % NY, col % NC
    h, z = row // ZS, row % ZS

    def partner(step):
        a, b, k = step
        return ((x + a) % NX) * (NY * NC) + ((y + b) % NY) * NC + (c + k) % NC

    def columns(p):
        return pl.ds(pl.multiple_of(p * COLS, 128), COLS)

    order = [partner(s) for s in STEPS] + [col]

    loads = {}
    for name, (src, dst) in enumerate(((g_hbm, g), (w_hbm, w), (m_hbm, m))):
        for i, p in enumerate(order):
            loads[name, i] = pltpu.make_async_copy(src.at[:, columns(p)], dst.at[p], load.at[name, i])
    for i in range(PEERS):
        loads[0, i].start()
    for i in range(PEERS):
        loads[1, i].start()
    for i in range(PEERS):
        loads[2, i].start()

    barrier = pltpu.get_barrier_semaphore()
    plane_ids = []
    for a, hh, b, k in PLANE:
        plane_ids.append({"row": ((h + hh) % 2) * ZS + z, "col": partner((a, b, k))})
    line_ids = [{"row": h * ZS + (z + d) % ZS, "col": col} for d in range(1, ZS)]
    for ids in plane_ids + line_ids:
        pl.semaphore_signal(barrier, inc=1, device_id=ids, device_id_type=MESH)

    acc = jnp.zeros((8, COLS), jnp.float32)
    for i, p in enumerate(order):
        loads[0, i].wait()
        for r in range(0, ROWS, 8):
            v = g[p, r : r + 8, :]
            acc = acc + v * v
    acc = jnp.sum(acc, axis=0, keepdims=True)
    own = acc[:, 0:128]
    for j in range(128, COLS, 128):
        own = own + acc[:, j : j + 128]
    part[0] = own
    place = row // ZS * PEERS + col
    plane[place] = own

    pl.semaphore_wait(barrier, len(PLANE) + ZS - 1)

    def plane_copy(j):
        return pltpu.make_async_remote_copy(
            src_ref=part.at[0], dst_ref=plane.at[place], send_sem=p_send.at[j], recv_sem=p_recv.at[j],
            device_id=plane_ids[j], device_id_type=MESH,
        )

    def block_copy(src, dst, send, recv, i):
        return pltpu.make_async_remote_copy(
            src_ref=src.at[order[i]], dst_ref=dst.at[pl.ds(pl.multiple_of(col * ROWS, ROWS), ROWS)],
            send_sem=send.at[i], recv_sem=recv.at[i],
            device_id={"col": order[i]}, device_id_type=MESH,
        )

    small = [plane_copy(j) for j in range(len(PLANE))]
    for copy in small:
        copy.start()
    w_copies = [block_copy(w, nw, w_send, w_recv, i) for i in range(PEERS - 1)]
    for i, copy in enumerate(w_copies):
        loads[1, i].wait()
        copy.start()
    loads[1, PEERS - 1].wait()

    for copy in small:
        copy.wait_recv()
    total = plane[0]
    for j in range(1, 2 * PEERS):
        total = total + plane[j]
    part[1] = total
    line[z] = total
    for i in range(PEERS):
        loads[2, i].wait()
    lines = [
        pltpu.make_async_remote_copy(
            src_ref=part.at[1], dst_ref=line.at[z], send_sem=z_send.at[d], recv_sem=z_recv.at[d],
            device_id=line_ids[d], device_id_type=MESH,
        )
        for d in range(ZS - 1)
    ]
    for copy in lines:
        copy.start()
    for copy in lines:
        copy.wait_recv()
    total = line[0]
    for j in range(1, ZS):
        total = total + line[j]
    total = jnp.sum(total, axis=1, keepdims=True)
    factor = jnp.minimum(jnp.float32(1.0), jnp.float32(LIMIT) / (jnp.sqrt(total) + jnp.float32(1e-06)))

    m_copies = [block_copy(out, nm, m_send, m_recv, i) for i in range(PEERS - 1)]
    for i, p in enumerate(order):
        out[p] = jnp.float32(0.9) * m[p] + factor * g[p]
        if i:
            m_copies[i - 1].start()

    here = pl.ds(pl.multiple_of(col * ROWS, ROWS), ROWS)
    mine = out[col]
    nm[here] = mine
    nw[here] = w[col] - jnp.float32(0.1) * mine
    for i, s in enumerate(STEPS):
        a, b, k = s
        src = partner((NX - a, NY - b, NC - k))
        rows = pl.ds(pl.multiple_of(src * ROWS, ROWS), ROWS)
        w_copies[i].wait_recv()
        m_copies[i].wait_recv()
        nw[rows] = nw[rows] - jnp.float32(0.1) * nm[rows]
    for copy in small + lines + w_copies + m_copies:
        copy.wait_send()


def body(grad, momentum, weight):
    f32 = jnp.float32
    dma = pltpu.SemaphoreType.DMA
    n = PEERS - 1
    blocks = pltpu.VMEM((PEERS, ROWS, COLS), f32)
    return pl.pallas_call(
        kernel,
        out_shape=[jax.ShapeDtypeStruct((PEERS * ROWS, COLS), f32)] * 2,
        in_specs=[pl.BlockSpec(memory_space=pltpu.HBM)] * 3,
        out_specs=[pl.BlockSpec(memory_space=pltpu.VMEM)] * 2,
        scratch_shapes=[
            blocks, blocks, blocks, blocks,
            pltpu.VMEM((2, 1, 128), f32),
            pltpu.VMEM((2 * PEERS, 1, 128), f32),
            pltpu.VMEM((ZS, 1, 128), f32),
            dma((3, PEERS)),
            dma((n,)), dma((n,)), dma((n,)), dma((n,)),
            dma((len(PLANE),)), dma((len(PLANE),)),
            dma((ZS - 1,)), dma((ZS - 1,)),
        ],
        compiler_params=pltpu.CompilerParams(
            collective_id=0, has_side_effects=True, vmem_limit_bytes=40 * 2**20
        ),
    )(grad, momentum, weight)


def solution(mesh):
    return jax.shard_map(
        body,
        mesh=mesh,
        in_specs=(P(("row", "col"), None),) * 3,
        out_specs=(P("row", "col"),) * 2,
        check_vma=False,
    )
```

```python
import math

import jax
import jax.numpy as jnp
from jax import lax
from jax.experimental import pallas as pl
from jax.experimental.pallas import tpu as pltpu
from jax.sharding import PartitionSpec as P

D = 8192
FF = 14336
MESH = pl.DeviceIdType.MESH
LIMIT = math.sqrt(D * FF)

NX, NY, NC = 4, 2, 2
NZ = 4
PEERS = NX * NY * NC
ROWS, COLS = 64, 896
PIECES = 8

STEPS = sorted(
    [(a, b, c) for a in range(NX) for b in range(NY) for c in range(NC) if a or b or c],
    key=lambda s: -min(s[0], NX - s[0]) - s[1],
)
FIRST = [(1, 0, 0), (3, 0, 0), (0, 1, 0)]
SPLIT = 32
NEAR = [(1, 0), (3, 0), (0, 1)]
MAIN = 1


def kernel(
    g_hbm, m_hbm, w_hbm, nw, nm, g, m, w, out, part, group, pair, final,
    load, f_send, f_recv, w_send, w_recv, m_send, m_recv, g_send, g_recv, p_send, p_recv, t_send, t_recv, ready,
):
    col, row = lax.axis_index("col"), lax.axis_index("row")
    x, y, c = col // (NY * NC), (col // NC) % NY, col % NC
    h, z = row // NZ, row % NZ

    def place(a, b, k):
        return ((x + a) % NX) * (NY * NC) + ((y + b) % NY) * NC + k

    def partner(step):
        a, b, k = step
        return place(a, b, (c + k) % NC)

    def columns(p):
        return pl.ds(pl.multiple_of(p * COLS, 128), COLS)

    def rows_of(p, start=0, size=ROWS):
        return pl.ds(pl.multiple_of(p * ROWS + start, 8), size)

    near = [{"col": place(a, b, MAIN)} for a, b in NEAR]
    other = {"col": place(0, 0, 1 - c)}
    outside = [
        {"row": (1 - h) * NZ + z, "col": partner((0, 1, 0))},
        {"row": h * NZ + z + 1 - 2 * (z % 2), "col": col},
        {"row": h * NZ + NZ - 1 - z, "col": col},
    ]

    barrier = pltpu.get_barrier_semaphore()
    for ids in near:
        pl.semaphore_signal(barrier, inc=1, device_id=ids, device_id_type=MESH)

    @pl.when(c != MAIN)
    def _():
        pl.semaphore_signal(barrier, inc=1, device_id=other, device_id_type=MESH)
        for ids in outside:
            pl.semaphore_signal(barrier, inc=1, device_id=ids, device_id_type=MESH)

    order = [partner(s) for s in STEPS] + [col]

    def loading(k, i):
        src, dst = ((g_hbm, g), (w_hbm, w), (m_hbm, m))[k]
        return pltpu.make_async_copy(src.at[:, columns(order[i])], dst.at[order[i]], load.at[k, i])

    begin = [STEPS.index(s) for s in FIRST]
    for i in begin:
        loading(1, i).start()
    for i in range(PEERS):
        loading(0, i).start()
    for i in range(PEERS):
        if i not in begin:
            loading(1, i).start()
    for i in range(PEERS):
        loading(2, i).start()

    def block_copy(src, dst, send, recv, i, start, size):
        return pltpu.make_async_remote_copy(
            src_ref=src.at[order[i], pl.ds(start, size)], dst_ref=dst.at[rows_of(col, start, size)],
            send_sem=send, recv_sem=recv, device_id={"col": order[i]}, device_id_type=MESH,
        )

    f_copies = [block_copy(w, nw, f_send.at[j], f_recv.at[j], i, 0, SPLIT) for j, i in enumerate(begin)]
    w_copies = []
    for i in range(PEERS - 1):
        start = SPLIT if i in begin else 0
        w_copies.append(block_copy(w, nw, w_send.at[i], w_recv.at[i], i, start, ROWS - start))
    m_copies = [block_copy(out, nm, m_send.at[i], m_recv.at[i], i, 0, ROWS) for i in range(PEERS - 1)]

    for i in begin:
        loading(1, i).wait()
    @pl.when(c == MAIN)
    def _():
        pl.semaphore_wait(barrier, 2 * len(NEAR) + 1)
        for ids in near:
            pl.semaphore_signal(ready.at[1], inc=1, device_id=ids, device_id_type=MESH)
        pl.semaphore_signal(ready.at[0], inc=1, device_id=other, device_id_type=MESH)

    @pl.when(c != MAIN)
    def _():
        pl.semaphore_wait(ready.at[0], 1)

    for copy in f_copies:
        copy.start()

    @pl.when(c == MAIN)
    def _():
        pl.semaphore_wait(ready.at[1], len(NEAR))
        for ids in near:
            pl.semaphore_signal(ready.at[2], inc=1, device_id=ids, device_id_type=MESH)

    acc = jnp.zeros((8, COLS), jnp.float32)
    for i, p in enumerate(order):
        loading(0, i).wait()
        for r in range(0, ROWS, 8):
            v = g[p, r : r + 8, :]
            acc = acc + v * v
    acc = jnp.sum(acc, axis=0, keepdims=True)
    own = acc[:, 0:128]
    for j in range(128, COLS, 128):
        own = own + acc[:, j : j + 128]
    part[0] = own
    group[col] = own

    @pl.when(c == MAIN)
    def _():
        pl.semaphore_wait(ready.at[2], len(NEAR))
        pl.semaphore_signal(ready.at[1], inc=1, device_id=other, device_id_type=MESH)

    @pl.when(c != MAIN)
    def _():
        pl.semaphore_wait(ready.at[1], 1)

    sums = [
        pltpu.make_async_remote_copy(
            src_ref=part.at[0], dst_ref=group.at[col], send_sem=g_send.at[i], recv_sem=g_recv.at[i],
            device_id={"col": order[i]}, device_id_type=MESH,
        )
        for i in range(PEERS - 1)
    ]
    for copy in sums:
        copy.start()
    for copy in sums:
        copy.wait_send()
    for i in range(PEERS - 1):
        if i not in begin:
            loading(1, i).wait()
        w_copies[i].start()
    loading(1, PEERS - 1).wait()

    for copy in sums:
        copy.wait_recv()
    total = group[0]
    for j in range(1, PEERS):
        total = total + group[j]
    for i in range(PEERS):
        loading(2, i).wait()

    told = pltpu.make_async_remote_copy(
        src_ref=part.at[4], dst_ref=final.at[0], send_sem=t_send.at[0], recv_sem=t_recv.at[0],
        device_id=other, device_id_type=MESH,
    )

    @pl.when(c != MAIN)
    def _():
        pl.semaphore_wait(barrier, len(outside))
        value = total
        copies = []
        for j, ids in enumerate(outside):
            part[1 + j] = value
            copy = pltpu.make_async_remote_copy(
                src_ref=part.at[1 + j], dst_ref=pair.at[j], send_sem=p_send.at[j], recv_sem=p_recv.at[j],
                device_id=ids, device_id_type=MESH,
            )
            copy.start()
            copies.append(copy)
            copy.wait_recv()
            value = value + pair[j]
        part[4] = value
        final[0] = value
        for copy in copies:
            copy.wait_send()
        told.start()
        told.wait_send()

    @pl.when(c == MAIN)
    def _():
        told.wait_recv()

    total = jnp.sum(final[0], axis=1, keepdims=True)
    factor = jnp.minimum(jnp.float32(1.0), jnp.float32(LIMIT) / (jnp.sqrt(total) + jnp.float32(1e-06)))

    for i, p in enumerate(order):
        out[p] = jnp.float32(0.9) * m[p] + factor * g[p]
        if i:
            m_copies[i - 1].start()

    mine = out[col]
    nm[rows_of(col)] = mine
    nw[rows_of(col)] = w[col] - jnp.float32(0.1) * mine
    for i, (a, b, k) in enumerate(STEPS):
        rows = rows_of(partner((NX - a, NY - b, NC - k)))
        if i in begin:
            f_copies[begin.index(i)].wait_recv()
        w_copies[i].wait_recv()
        m_copies[i].wait_recv()
        nw[rows] = nw[rows] - jnp.float32(0.1) * nm[rows]
    for copy in f_copies + w_copies + m_copies:
        copy.wait_send()


def store(nw, nm, nw_hbm, nm_hbm, sem):
    size = nw.shape[0] // PIECES
    copies = []
    for k, (src, dst) in enumerate(((nw, nw_hbm), (nm, nm_hbm))):
        for i in range(PIECES):
            rows = pl.ds(i * size, size)
            copies.append(pltpu.make_async_copy(src.at[rows], dst.at[rows], sem.at[k, i]))
    for copy in copies:
        copy.start()
    for copy in copies:
        copy.wait()


def body(grad, momentum, weight):
    f32 = jnp.float32
    dma = pltpu.SemaphoreType.DMA
    n = PEERS - 1
    blocks = pltpu.VMEM((PEERS, ROWS, COLS), f32)
    outs = [jax.ShapeDtypeStruct((PEERS * ROWS, COLS), f32)] * 2
    landed = pl.pallas_call(
        kernel,
        out_shape=outs,
        in_specs=[pl.BlockSpec(memory_space=pl.ANY)] * 3,
        out_specs=[pl.BlockSpec(memory_space=pltpu.VMEM)] * 2,
        scratch_shapes=[
            blocks, blocks, blocks, blocks,
            pltpu.VMEM((5, 1, 128), f32),
            pltpu.VMEM((PEERS, 1, 128), f32),
            pltpu.VMEM((3, 1, 128), f32),
            pltpu.VMEM((1, 1, 128), f32),
            dma((3, PEERS)),
            dma((len(FIRST),)), dma((len(FIRST),)),
            dma((n,)), dma((n,)), dma((n,)), dma((n,)), dma((n,)), dma((n,)),
            dma((3,)), dma((3,)), dma((1,)), dma((1,)),
            pltpu.SemaphoreType.REGULAR((3,)),
        ],
        compiler_params=pltpu.CompilerParams(
            collective_id=0, has_side_effects=True, vmem_limit_bytes=45 * 2**20
        ),
    )(grad, momentum, weight)
    return pl.pallas_call(
        store,
        out_shape=outs,
        in_specs=[pl.BlockSpec(memory_space=pltpu.VMEM)] * 2,
        out_specs=[pl.BlockSpec(memory_space=pl.ANY)] * 2,
        scratch_shapes=[dma((2, PIECES))],
        compiler_params=pltpu.CompilerParams(vmem_limit_bytes=2 * 2**20),
    )(*landed)


def solution(mesh):
    return jax.shard_map(
        body,
        mesh=mesh,
        in_specs=(P(("row", "col"), None),) * 3,
        out_specs=(P("row", "col"),) * 2,
        check_vma=False,
    )
```

```python
import math

import jax
import jax.numpy as jnp
from jax import lax
from jax.experimental import pallas as pl
from jax.experimental.pallas import tpu as pltpu
from jax.sharding import PartitionSpec as P

D = 8192
FF = 14336
MESH = pl.DeviceIdType.MESH
LIMIT = math.sqrt(D * FF)

NX, NY, NC = 4, 2, 2
NZ = 4
PEERS = NX * NY * NC
ROWS, COLS = 64, 896
PIECES = 8

STEPS = sorted(
    [(a, b, c) for a in range(NX) for b in range(NY) for c in range(NC) if a or b or c],
    key=lambda s: -min(s[0], NX - s[0]) - s[1],
)
FIRST = [(1, 0, 0), (3, 0, 0), (0, 1, 0)]
SPLIT = 32
NEAR = [(1, 0), (3, 0), (0, 1)]
MAIN = 1
LOADS = 4


def kernel(
    g_hbm, m_hbm, w_hbm, nw, nm, g, m, w, out, part, group, pair, final,
    load, send, recv, p_send, p_recv, t_send, t_recv, ready,
):
    col, row = lax.axis_index("col"), lax.axis_index("row")
    x, y, c = col // (NY * NC), (col // NC) % NY, col % NC
    h, z = row // NZ, row % NZ

    def place(a, b, k):
        return ((x + a) % NX) * (NY * NC) + ((y + b) % NY) * NC + k

    def partner(step):
        a, b, k = step
        return place(a, b, (c + k) % NC)

    def columns(p):
        return pl.ds(pl.multiple_of(p * COLS, 128), COLS)

    def rows_of(p, start=0, size=ROWS):
        return pl.ds(pl.multiple_of(p * ROWS + start, 8), size)

    def wait_for(ref, sem):
        pltpu.make_async_copy(ref, ref, sem).wait()

    near = [{"col": place(a, b, MAIN)} for a, b in NEAR]
    other = {"col": place(0, 0, 1 - c)}
    outside = [
        {"row": (1 - h) * NZ + z, "col": partner((0, 1, 0))},
        {"row": h * NZ + z + 1 - 2 * (z % 2), "col": col},
        {"row": h * NZ + NZ - 1 - z, "col": col},
    ]

    barrier = pltpu.get_barrier_semaphore()
    for ids in near:
        pl.semaphore_signal(barrier, inc=1, device_id=ids, device_id_type=MESH)

    @pl.when(c != MAIN)
    def _():
        pl.semaphore_signal(barrier, inc=1, device_id=other, device_id_type=MESH)
        for ids in outside:
            pl.semaphore_signal(barrier, inc=1, device_id=ids, device_id_type=MESH)

    order = [partner(s) for s in STEPS] + [col]
    begin = [STEPS.index(s) for s in FIRST]
    later = [i for i in range(PEERS) if i not in begin]

    def load_rows(src, dst, k):
        size = ROWS // LOADS
        for j in range(LOADS):
            rows = pl.ds(j * size, size)
            pltpu.make_async_copy(src.at[rows], dst.at[rows], load.at[k]).start()

    for i in begin:
        pltpu.make_async_copy(w_hbm.at[:, columns(order[i])], w.at[order[i]], load.at[0]).start()
    load_rows(g_hbm, g, 1)
    for i in later:
        pltpu.make_async_copy(w_hbm.at[:, columns(order[i])], w.at[order[i]], load.at[2]).start()
    load_rows(m_hbm, m, 3)

    def block_copy(src, dst, k, i, start=0, size=ROWS):
        return pltpu.make_async_remote_copy(
            src_ref=src.at[order[i], pl.ds(start, size)], dst_ref=dst.at[rows_of(col, start, size)],
            send_sem=send.at[k], recv_sem=recv.at[k], device_id={"col": order[i]}, device_id_type=MESH,
        )

    wait_for(w.at[pl.ds(0, len(begin))], load.at[0])

    @pl.when(c == MAIN)
    def _():
        pl.semaphore_wait(barrier, 2 * len(NEAR) + 1)
        for ids in near:
            pl.semaphore_signal(ready.at[1], inc=1, device_id=ids, device_id_type=MESH)
        pl.semaphore_signal(ready.at[0], inc=1, device_id=other, device_id_type=MESH)

    @pl.when(c != MAIN)
    def _():
        pl.semaphore_wait(ready.at[0], 1)

    for i in begin:
        block_copy(w, nw, 0, i, 0, SPLIT).start()

    @pl.when(c == MAIN)
    def _():
        pl.semaphore_wait(ready.at[1], len(NEAR))
        for ids in near:
            pl.semaphore_signal(ready.at[2], inc=1, device_id=ids, device_id_type=MESH)

    wait_for(g, load.at[1])
    acc = jnp.zeros((8, COLS), jnp.float32)
    for i in range(PEERS):
        for r in range(0, ROWS, 8):
            v = g[r : r + 8, i * COLS : (i + 1) * COLS]
            acc = acc + v * v
    acc = jnp.sum(acc, axis=0, keepdims=True)
    own = acc[:, 0:128]
    for j in range(128, COLS, 128):
        own = own + acc[:, j : j + 128]
    part[0] = own
    group[col] = own

    @pl.when(c == MAIN)
    def _():
        pl.semaphore_wait(ready.at[2], len(NEAR))
        pl.semaphore_signal(ready.at[1], inc=1, device_id=other, device_id_type=MESH)

    @pl.when(c != MAIN)
    def _():
        pl.semaphore_wait(ready.at[1], 1)

    for i in range(PEERS - 1):
        pltpu.make_async_remote_copy(
            src_ref=part.at[0], dst_ref=group.at[col], send_sem=send.at[2], recv_sem=recv.at[2],
            device_id={"col": order[i]}, device_id_type=MESH,
        ).start()
    wait_for(group.at[pl.ds(0, PEERS - 1)], send.at[2])
    wait_for(w.at[pl.ds(0, len(later))], load.at[2])

    def send_weight():
        for i in range(PEERS - 1):
            start = SPLIT if i in begin else 0
            if start < ROWS:
                block_copy(w, nw, 0, i, start, ROWS - start).start()

    send_weight()
    wait_for(group.at[pl.ds(0, PEERS - 1)], recv.at[2])
    total = group[0]
    for j in range(1, PEERS):
        total = total + group[j]

    told = pltpu.make_async_remote_copy(
        src_ref=part.at[4], dst_ref=final.at[0], send_sem=t_send, recv_sem=t_recv,
        device_id=other, device_id_type=MESH,
    )

    @pl.when(c != MAIN)
    def _():
        pl.semaphore_wait(barrier, len(outside))
        value = total
        for j, ids in enumerate(outside):
            part[1 + j] = value
            copy = pltpu.make_async_remote_copy(
                src_ref=part.at[1 + j], dst_ref=pair.at[j], send_sem=p_send.at[j], recv_sem=p_recv.at[j],
                device_id=ids, device_id_type=MESH,
            )
            copy.start()
            copy.wait()
            value = value + pair[j]
        part[4] = value
        final[0] = value
        told.start()
        told.wait_send()

    @pl.when(c == MAIN)
    def _():
        told.wait_recv()

    total = jnp.sum(final[0], axis=1, keepdims=True)
    factor = jnp.minimum(jnp.float32(1.0), jnp.float32(LIMIT) / (jnp.sqrt(total) + jnp.float32(1e-06)))

    wait_for(m, load.at[3])
    for i, p in enumerate(order):
        out[p] = jnp.float32(0.9) * m[:, columns(p)] + factor * g[:, columns(p)]
        if i:
            block_copy(out, nm, 1, i - 1).start()

    nm[rows_of(col)] = out[col]
    nw[rows_of(col)] = w[col]
    for k, ref in enumerate((nw, nm)):
        wait_for(ref.at[pl.ds(0, (PEERS - 1) * ROWS)], recv.at[k])
    for k, ref in enumerate((nw, nm)):
        wait_for(ref.at[pl.ds(0, (PEERS - 1) * ROWS)], send.at[k])


def store(w, nm, nw_hbm, nm_hbm, nw, sem):
    size = w.shape[0] // PIECES

    def piece(src, dst, k, i):
        rows = pl.ds(i * size, size)
        return pltpu.make_async_copy(src.at[rows], dst.at[rows], sem.at[k])

    for i in range(PIECES):
        piece(nm, nm_hbm, 0, i).start()
    for i in range(PIECES):
        rows = pl.ds(i * size, size)
        nw[rows] = w[rows] - jnp.float32(0.1) * nm[rows]
        if i:
            piece(nw, nw_hbm, 1, i - 1).start()
    piece(nw, nw_hbm, 1, PIECES - 1).start()
    pltpu.make_async_copy(nm, nm_hbm, sem.at[0]).wait()
    pltpu.make_async_copy(nw, nw_hbm, sem.at[1]).wait()


def body(grad, momentum, weight):
    f32 = jnp.float32
    dma = pltpu.SemaphoreType.DMA
    blocks = pltpu.VMEM((PEERS, ROWS, COLS), f32)
    whole = pltpu.VMEM((ROWS, PEERS * COLS), f32)
    outs = [jax.ShapeDtypeStruct((PEERS * ROWS, COLS), f32)] * 2
    landed = pl.pallas_call(
        kernel,
        out_shape=outs,
        in_specs=[pl.BlockSpec(memory_space=pl.ANY)] * 3,
        out_specs=[pl.BlockSpec(memory_space=pltpu.VMEM)] * 2,
        scratch_shapes=[
            whole, whole, blocks, blocks,
            pltpu.VMEM((5, 1, 128), f32),
            pltpu.VMEM((PEERS, 1, 128), f32),
            pltpu.VMEM((3, 1, 128), f32),
            pltpu.VMEM((1, 1, 128), f32),
            dma((4,)), dma((3,)), dma((3,)), dma((3,)), dma((3,)), dma, dma,
            pltpu.SemaphoreType.REGULAR((3,)),
        ],
        compiler_params=pltpu.CompilerParams(
            collective_id=0, has_side_effects=True, vmem_limit_bytes=45 * 2**20
        ),
    )(grad, momentum, weight)
    return pl.pallas_call(
        store,
        out_shape=outs,
        in_specs=[pl.BlockSpec(memory_space=pltpu.VMEM)] * 2,
        out_specs=[pl.BlockSpec(memory_space=pl.ANY)] * 2,
        scratch_shapes=[pltpu.VMEM((PEERS * ROWS, COLS), f32), dma((2,))],
        compiler_params=pltpu.CompilerParams(vmem_limit_bytes=8 * 2**20),
    )(*landed)


def solution(mesh):
    return jax.shard_map(
        body,
        mesh=mesh,
        in_specs=(P(("row", "col"), None),) * 3,
        out_specs=(P("row", "col"),) * 2,
        check_vma=False,
    )
```

```python
import math

import jax
import jax.numpy as jnp
from jax import lax
from jax.experimental import pallas as pl
from jax.experimental.pallas import tpu as pltpu
from jax.sharding import PartitionSpec as P

D = 8192
FF = 14336
MESH = pl.DeviceIdType.MESH
LIMIT = math.sqrt(D * FF)

NX, NY, NC = 4, 2, 2
NZ = 4
PEERS = NX * NY * NC
ROWS, COLS = 64, 896
PIECES = 8

STEPS = [
    (2, 1, 1), (2, 1, 0), (1, 1, 1), (1, 1, 0), (2, 0, 1), (2, 0, 0), (3, 1, 1), (3, 1, 0),
    (0, 1, 1), (0, 1, 0), (1, 0, 1), (1, 0, 0), (3, 0, 1), (3, 0, 0), (0, 0, 1),
]
FIRST = [(1, 0, 0), (3, 0, 0), (0, 1, 0)]
SECOND = [(0, 1, 1), (1, 0, 1), (3, 0, 1), (0, 0, 1)]
THIRD = STEPS[:8]
NEAR = [(1, 0), (3, 0), (0, 1)]
MAIN = 1
LOADS = 4


def kernel(
    g_hbm, m_hbm, w_hbm, nw, nm, g, m, w, out, part, group, pair, final,
    load, send, recv, p_send, p_recv, t_send, t_recv, ready,
):
    col, row = lax.axis_index("col"), lax.axis_index("row")
    x, y, c = col // (NY * NC), (col // NC) % NY, col % NC
    h, z = row // NZ, row % NZ

    def place(a, b, k):
        return ((x + a) % NX) * (NY * NC) + ((y + b) % NY) * NC + k

    def partner(step):
        a, b, k = step
        return place(a, b, (c + k) % NC)

    def columns(p):
        return pl.ds(pl.multiple_of(p * COLS, 128), COLS)

    def rows_of(p):
        return pl.ds(pl.multiple_of(p * ROWS, ROWS), ROWS)

    def wait_for(ref, sem):
        pltpu.make_async_copy(ref, ref, sem).wait()

    near = [{"col": place(a, b, MAIN)} for a, b in NEAR]
    other = {"col": place(0, 0, 1 - c)}
    outside = [
        {"row": (1 - h) * NZ + z, "col": partner((0, 1, 0))},
        {"row": h * NZ + z + 1 - 2 * (z % 2), "col": col},
        {"row": h * NZ + NZ - 1 - z, "col": col},
    ]

    barrier = pltpu.get_barrier_semaphore()
    for ids in near:
        pl.semaphore_signal(barrier, inc=1, device_id=ids, device_id_type=MESH)

    @pl.when(c != MAIN)
    def _():
        pl.semaphore_signal(barrier, inc=1, device_id=other, device_id_type=MESH)
        for ids in outside:
            pl.semaphore_signal(barrier, inc=1, device_id=ids, device_id_type=MESH)

    order = [partner(s) for s in STEPS] + [col]
    first, second, third = ([STEPS.index(s) for s in part_of] for part_of in (FIRST, SECOND, THIRD))
    later = second + third + [PEERS - 1]

    def load_rows(src, dst, k):
        size = ROWS // LOADS
        for j in range(LOADS):
            rows = pl.ds(j * size, size)
            pltpu.make_async_copy(src.at[rows], dst.at[rows], load.at[k]).start()

    for i in first:
        pltpu.make_async_copy(w_hbm.at[:, columns(order[i])], w.at[order[i]], load.at[0]).start()
    load_rows(g_hbm, g, 1)

    def block_copy(src, dst, k, i):
        return pltpu.make_async_remote_copy(
            src_ref=src.at[order[i]], dst_ref=dst.at[rows_of(col)],
            send_sem=send.at[k], recv_sem=recv.at[k], device_id={"col": order[i]}, device_id_type=MESH,
        )

    wait_for(w.at[pl.ds(0, len(first))], load.at[0])

    @pl.when(c == MAIN)
    def _():
        pl.semaphore_wait(barrier, 2 * len(NEAR) + 1)
        for ids in near:
            pl.semaphore_signal(ready.at[1], inc=1, device_id=ids, device_id_type=MESH)
        pl.semaphore_signal(ready.at[0], inc=1, device_id=other, device_id_type=MESH)

    @pl.when(c != MAIN)
    def _():
        pl.semaphore_wait(ready.at[0], 1)

    for i in first:
        block_copy(w, nw, 0, i).start()
    for i in later:
        pltpu.make_async_copy(w_hbm.at[:, columns(order[i])], w.at[order[i]], load.at[2]).start()
    load_rows(m_hbm, m, 3)

    @pl.when(c == MAIN)
    def _():
        pl.semaphore_wait(ready.at[1], len(NEAR))
        for ids in near:
            pl.semaphore_signal(ready.at[2], inc=1, device_id=ids, device_id_type=MESH)

    wait_for(g, load.at[1])
    acc = jnp.zeros((8, COLS), jnp.float32)
    for i in range(PEERS):
        for r in range(0, ROWS, 8):
            v = g[r : r + 8, i * COLS : (i + 1) * COLS]
            acc = acc + v * v
    acc = jnp.sum(acc, axis=0, keepdims=True)
    own = acc[:, 0:128]
    for j in range(128, COLS, 128):
        own = own + acc[:, j : j + 128]
    part[0] = own
    group[col] = own

    @pl.when(c == MAIN)
    def _():
        pl.semaphore_wait(ready.at[2], len(NEAR))
        pl.semaphore_signal(ready.at[1], inc=1, device_id=other, device_id_type=MESH)

    @pl.when(c != MAIN)
    def _():
        pl.semaphore_wait(ready.at[1], 1)

    for i in range(PEERS - 1):
        pltpu.make_async_remote_copy(
            src_ref=part.at[0], dst_ref=group.at[col], send_sem=send.at[2], recv_sem=recv.at[2],
            device_id={"col": order[i]}, device_id_type=MESH,
        ).start()
    wait_for(group.at[pl.ds(0, PEERS - 1)], send.at[2])
    wait_for(w.at[pl.ds(0, len(later))], load.at[2])

    for i in second:
        block_copy(w, nw, 0, i).start()

    wait_for(group.at[pl.ds(0, PEERS - 1)], recv.at[2])
    for i in third:
        block_copy(w, nw, 0, i).start()

    total = group[0]
    for j in range(1, PEERS):
        total = total + group[j]

    told = pltpu.make_async_remote_copy(
        src_ref=part.at[4], dst_ref=final.at[0], send_sem=t_send, recv_sem=t_recv,
        device_id=other, device_id_type=MESH,
    )

    @pl.when(c != MAIN)
    def _():
        pl.semaphore_wait(barrier, len(outside))
        value = total
        for j, ids in enumerate(outside):
            part[1 + j] = value
            copy = pltpu.make_async_remote_copy(
                src_ref=part.at[1 + j], dst_ref=pair.at[j], send_sem=p_send.at[j], recv_sem=p_recv.at[j],
                device_id=ids, device_id_type=MESH,
            )
            copy.start()
            copy.wait()
            value = value + pair[j]
        part[4] = value
        final[0] = value
        told.start()
        told.wait_send()

    @pl.when(c == MAIN)
    def _():
        told.wait_recv()

    total = jnp.sum(final[0], axis=1, keepdims=True)
    factor = jnp.minimum(jnp.float32(1.0), jnp.float32(LIMIT) / (jnp.sqrt(total) + jnp.float32(1e-06)))

    wait_for(m, load.at[3])
    for i, p in enumerate(order):
        out[p] = jnp.float32(0.9) * m[:, columns(p)] + factor * g[:, columns(p)]
        if i:
            block_copy(out, nm, 1, i - 1).start()

    nm[rows_of(col)] = out[col]
    nw[rows_of(col)] = w[col]
    for k, ref in enumerate((nw, nm)):
        wait_for(ref.at[pl.ds(0, (PEERS - 1) * ROWS)], recv.at[k])
    for k, ref in enumerate((nw, nm)):
        wait_for(ref.at[pl.ds(0, (PEERS - 1) * ROWS)], send.at[k])


def store(w, nm, nw_hbm, nm_hbm, nw, sem):
    size = w.shape[0] // PIECES

    def piece(src, dst, k, i):
        rows = pl.ds(i * size, size)
        return pltpu.make_async_copy(src.at[rows], dst.at[rows], sem.at[k])

    for i in range(PIECES):
        piece(nm, nm_hbm, 0, i).start()
    for i in range(PIECES):
        rows = pl.ds(i * size, size)
        nw[rows] = w[rows] - jnp.float32(0.1) * nm[rows]
        if i:
            piece(nw, nw_hbm, 1, i - 1).start()
    piece(nw, nw_hbm, 1, PIECES - 1).start()
    pltpu.make_async_copy(nm, nm_hbm, sem.at[0]).wait()
    pltpu.make_async_copy(nw, nw_hbm, sem.at[1]).wait()


def body(grad, momentum, weight):
    f32 = jnp.float32
    dma = pltpu.SemaphoreType.DMA
    blocks = pltpu.VMEM((PEERS, ROWS, COLS), f32)
    whole = pltpu.VMEM((ROWS, PEERS * COLS), f32)
    outs = [jax.ShapeDtypeStruct((PEERS * ROWS, COLS), f32)] * 2
    landed = pl.pallas_call(
        kernel,
        out_shape=outs,
        in_specs=[pl.BlockSpec(memory_space=pl.ANY)] * 3,
        out_specs=[pl.BlockSpec(memory_space=pltpu.VMEM)] * 2,
        scratch_shapes=[
            whole, whole, blocks, blocks,
            pltpu.VMEM((5, 1, 128), f32),
            pltpu.VMEM((PEERS, 1, 128), f32),
            pltpu.VMEM((3, 1, 128), f32),
            pltpu.VMEM((1, 1, 128), f32),
            dma((4,)), dma((3,)), dma((3,)), dma((3,)), dma((3,)), dma, dma,
            pltpu.SemaphoreType.REGULAR((3,)),
        ],
        compiler_params=pltpu.CompilerParams(
            collective_id=0, has_side_effects=True, vmem_limit_bytes=45 * 2**20
        ),
    )(grad, momentum, weight)
    return pl.pallas_call(
        store,
        out_shape=outs,
        in_specs=[pl.BlockSpec(memory_space=pltpu.VMEM)] * 2,
        out_specs=[pl.BlockSpec(memory_space=pl.ANY)] * 2,
        scratch_shapes=[pltpu.VMEM((PEERS * ROWS, COLS), f32), dma((2,))],
        compiler_params=pltpu.CompilerParams(vmem_limit_bytes=8 * 2**20),
    )(*landed)


def solution(mesh):
    return jax.shard_map(
        body,
        mesh=mesh,
        in_specs=(P(("row", "col"), None),) * 3,
        out_specs=(P("row", "col"),) * 2,
        check_vma=False,
    )
```

```python
import math

import jax
import jax.numpy as jnp
from jax import lax
from jax.experimental import pallas as pl
from jax.experimental.pallas import tpu as pltpu
from jax.sharding import PartitionSpec as P

D = 8192
FF = 14336
MESH = pl.DeviceIdType.MESH
LIMIT = math.sqrt(D * FF)

NX, NY, NC = 4, 2, 2
NZ = 4
PEERS = NX * NY * NC
ROWS, COLS = 64, 896
PIECES = 8

STEPS = [
    (2, 1, 1), (2, 1, 0), (1, 1, 1), (1, 1, 0), (2, 0, 1), (2, 0, 0), (3, 1, 1), (3, 1, 0),
    (0, 1, 1), (0, 1, 0), (1, 0, 1), (1, 0, 0), (3, 0, 1), (3, 0, 0), (0, 0, 1),
]
FIRST = [(1, 0, 0), (3, 0, 0), (0, 1, 0)]
SECOND = [(0, 1, 1), (1, 0, 1), (3, 0, 1), (0, 0, 1)]
THIRD = STEPS[:8]
NEAR = [(1, 0), (3, 0), (0, 1)]
MAIN = 1
LOADS = 4


def kernel(
    g_hbm, m_hbm, w_hbm, nw, nm, g, m, w, out, part, group, pair, final,
    load, send, recv, p_send, p_recv, t_send, t_recv, ready,
):
    col, row = lax.axis_index("col"), lax.axis_index("row")
    x, y, c = col // (NY * NC), (col // NC) % NY, col % NC
    h, z = row // NZ, row % NZ

    def place(a, b, k):
        return ((x + a) % NX) * (NY * NC) + ((y + b) % NY) * NC + k

    def partner(step):
        a, b, k = step
        return place(a, b, (c + k) % NC)

    def columns(p):
        return pl.ds(pl.multiple_of(p * COLS, 128), COLS)

    def rows_of(p):
        return pl.ds(pl.multiple_of(p * ROWS, ROWS), ROWS)

    def wait_for(ref, sem):
        pltpu.make_async_copy(ref, ref, sem).wait()

    near = [{"col": place(a, b, c)} for a, b in NEAR]
    other = {"col": place(0, 0, 1 - c)}
    outside = [
        {"row": (1 - h) * NZ + z, "col": partner((0, 1, 0))},
        {"row": h * NZ + z + 1 - 2 * (z % 2), "col": col},
        {"row": h * NZ + NZ - 1 - z, "col": col},
    ]

    asks = [h == 0, z % 2 == 0, z < NZ // 2]
    asked = h + z % 2 + z // (NZ // 2)

    barrier = pltpu.get_barrier_semaphore()
    for ids in near:
        pl.semaphore_signal(barrier, inc=1, device_id=ids, device_id_type=MESH)

    @pl.when(c == MAIN)
    def _():
        pl.semaphore_signal(barrier, inc=1, device_id=other, device_id_type=MESH)

    for ask, ids in zip(asks, outside):

        @pl.when((c != MAIN) & ask)
        def _():
            pl.semaphore_signal(barrier, inc=1, device_id=ids, device_id_type=MESH)

    order = [partner(s) for s in STEPS] + [col]
    first, second, third = ([STEPS.index(s) for s in part_of] for part_of in (FIRST, SECOND, THIRD))
    later = second + third + [PEERS - 1]

    def load_rows(src, dst, k):
        size = ROWS // LOADS
        for j in range(LOADS):
            rows = pl.ds(j * size, size)
            pltpu.make_async_copy(src.at[rows], dst.at[rows], load.at[k]).start()

    for i in first:
        pltpu.make_async_copy(w_hbm.at[:, columns(order[i])], w.at[order[i]], load.at[0]).start()
    load_rows(g_hbm, g, 1)

    def block_copy(src, dst, k, i):
        return pltpu.make_async_remote_copy(
            src_ref=src.at[order[i]], dst_ref=dst.at[rows_of(col)],
            send_sem=send.at[k], recv_sem=recv.at[k], device_id={"col": order[i]}, device_id_type=MESH,
        )

    wait_for(w.at[pl.ds(0, len(first))], load.at[0])

    @pl.when(c == MAIN)
    def _():
        pl.semaphore_wait(barrier, len(NEAR))

    @pl.when(c != MAIN)
    def _():
        pl.semaphore_wait(barrier, len(NEAR) + 1 + asked)
        pl.semaphore_signal(ready.at[0], inc=1, device_id=other, device_id_type=MESH)

    for i in first:
        block_copy(w, nw, 0, i).start()
    for i in later:
        pltpu.make_async_copy(w_hbm.at[:, columns(order[i])], w.at[order[i]], load.at[2]).start()
    load_rows(m_hbm, m, 3)

    @pl.when(c == MAIN)
    def _():
        pl.semaphore_wait(ready.at[0], 1)
        for ids in near:
            pl.semaphore_signal(ready.at[1], inc=1, device_id=ids, device_id_type=MESH)
        pl.semaphore_wait(ready.at[1], len(NEAR))
        for ids in near:
            pl.semaphore_signal(ready.at[2], inc=1, device_id=ids, device_id_type=MESH)

    for j, (ask, ids) in enumerate(zip(asks, outside)):

        @pl.when((c != MAIN) & jnp.logical_not(ask))
        def _():
            pl.semaphore_signal(ready.at[3 + j], inc=1, device_id=ids, device_id_type=MESH)

    wait_for(g, load.at[1])
    acc = jnp.zeros((8, COLS), jnp.float32)
    for i in range(PEERS):
        for r in range(0, ROWS, 8):
            v = g[r : r + 8, i * COLS : (i + 1) * COLS]
            acc = acc + v * v
    acc = jnp.sum(acc, axis=0, keepdims=True)
    own = acc[:, 0:128]
    for j in range(128, COLS, 128):
        own = own + acc[:, j : j + 128]
    part[0] = own
    group[col] = own

    @pl.when(c == MAIN)
    def _():
        pl.semaphore_wait(ready.at[2], len(NEAR))
        pl.semaphore_signal(ready.at[1], inc=1, device_id=other, device_id_type=MESH)

    @pl.when(c != MAIN)
    def _():
        pl.semaphore_wait(ready.at[1], 1)

    for i in range(PEERS - 1):
        pltpu.make_async_remote_copy(
            src_ref=part.at[0], dst_ref=group.at[col], send_sem=send.at[2], recv_sem=recv.at[2],
            device_id={"col": order[i]}, device_id_type=MESH,
        ).start()
    wait_for(group.at[pl.ds(0, PEERS - 1)], send.at[2])
    wait_for(w.at[pl.ds(0, len(later))], load.at[2])

    for i in second:
        block_copy(w, nw, 0, i).start()

    wait_for(group.at[pl.ds(0, PEERS - 1)], recv.at[2])
    for i in third:
        block_copy(w, nw, 0, i).start()

    total = group[0]
    for j in range(1, PEERS):
        total = total + group[j]

    told = pltpu.make_async_remote_copy(
        src_ref=part.at[4], dst_ref=final.at[0], send_sem=t_send, recv_sem=t_recv,
        device_id=other, device_id_type=MESH,
    )

    @pl.when(c != MAIN)
    def _():
        value = total
        for j, ids in enumerate(outside):
            part[1 + j] = value

            @pl.when(asks[j])
            def _():
                pl.semaphore_wait(ready.at[3 + j], 1)

            copy = pltpu.make_async_remote_copy(
                src_ref=part.at[1 + j], dst_ref=pair.at[j], send_sem=p_send.at[j], recv_sem=p_recv.at[j],
                device_id=ids, device_id_type=MESH,
            )
            copy.start()
            copy.wait()
            value = value + pair[j]
        part[4] = value
        final[0] = value
        told.start()
        told.wait_send()

    @pl.when(c == MAIN)
    def _():
        told.wait_recv()

    total = jnp.sum(final[0], axis=1, keepdims=True)
    factor = jnp.minimum(jnp.float32(1.0), jnp.float32(LIMIT) / (jnp.sqrt(total) + jnp.float32(1e-06)))

    wait_for(m, load.at[3])
    for i, p in enumerate(order):
        out[p] = jnp.float32(0.9) * m[:, columns(p)] + factor * g[:, columns(p)]
        if i:
            block_copy(out, nm, 1, i - 1).start()

    nm[rows_of(col)] = out[col]
    nw[rows_of(col)] = w[col]
    for k, ref in enumerate((nw, nm)):
        wait_for(ref.at[pl.ds(0, (PEERS - 1) * ROWS)], recv.at[k])
    for k, ref in enumerate((nw, nm)):
        wait_for(ref.at[pl.ds(0, (PEERS - 1) * ROWS)], send.at[k])


def store(w, nm, nw_hbm, nm_hbm, nw, sem):
    size = w.shape[0] // PIECES

    def piece(src, dst, k, i):
        rows = pl.ds(i * size, size)
        return pltpu.make_async_copy(src.at[rows], dst.at[rows], sem.at[k])

    for i in range(PIECES):
        piece(nm, nm_hbm, 0, i).start()
    for i in range(PIECES):
        rows = pl.ds(i * size, size)
        nw[rows] = w[rows] - jnp.float32(0.1) * nm[rows]
        if i:
            piece(nw, nw_hbm, 1, i - 1).start()
    piece(nw, nw_hbm, 1, PIECES - 1).start()
    pltpu.make_async_copy(nm, nm_hbm, sem.at[0]).wait()
    pltpu.make_async_copy(nw, nw_hbm, sem.at[1]).wait()


def body(grad, momentum, weight):
    f32 = jnp.float32
    dma = pltpu.SemaphoreType.DMA
    blocks = pltpu.VMEM((PEERS, ROWS, COLS), f32)
    whole = pltpu.VMEM((ROWS, PEERS * COLS), f32)
    outs = [jax.ShapeDtypeStruct((PEERS * ROWS, COLS), f32)] * 2
    landed = pl.pallas_call(
        kernel,
        out_shape=outs,
        in_specs=[pl.BlockSpec(memory_space=pl.ANY)] * 3,
        out_specs=[pl.BlockSpec(memory_space=pltpu.VMEM)] * 2,
        scratch_shapes=[
            whole, whole, blocks, blocks,
            pltpu.VMEM((5, 1, 128), f32),
            pltpu.VMEM((PEERS, 1, 128), f32),
            pltpu.VMEM((3, 1, 128), f32),
            pltpu.VMEM((1, 1, 128), f32),
            dma((4,)), dma((3,)), dma((3,)), dma((3,)), dma((3,)), dma, dma,
            pltpu.SemaphoreType.REGULAR((6,)),
        ],
        compiler_params=pltpu.CompilerParams(
            collective_id=0, has_side_effects=True, vmem_limit_bytes=45 * 2**20
        ),
    )(grad, momentum, weight)
    return pl.pallas_call(
        store,
        out_shape=outs,
        in_specs=[pl.BlockSpec(memory_space=pltpu.VMEM)] * 2,
        out_specs=[pl.BlockSpec(memory_space=pl.ANY)] * 2,
        scratch_shapes=[pltpu.VMEM((PEERS * ROWS, COLS), f32), dma((2,))],
        compiler_params=pltpu.CompilerParams(vmem_limit_bytes=8 * 2**20),
    )(*landed)


def solution(mesh):
    return jax.shard_map(
        body,
        mesh=mesh,
        in_specs=(P(("row", "col"), None),) * 3,
        out_specs=(P("row", "col"),) * 2,
        check_vma=False,
    )
```

```python
import math

import jax
import jax.numpy as jnp
from jax import lax
from jax.experimental import pallas as pl
from jax.experimental.pallas import tpu as pltpu
from jax.sharding import PartitionSpec as P

D = 8192
FF = 14336
MESH = pl.DeviceIdType.MESH
LIMIT = math.sqrt(D * FF)

NX, NY, NC = 4, 2, 2
NZ = 4
PEERS = NX * NY * NC
ROWS, COLS = 64, 896
PIECES = 8

STEPS = [
    (2, 1, 1), (2, 1, 0), (1, 1, 1), (1, 1, 0), (2, 0, 1), (2, 0, 0), (3, 1, 1), (3, 1, 0),
    (0, 1, 1), (0, 1, 0), (1, 0, 1), (1, 0, 0), (3, 0, 1), (3, 0, 0), (0, 0, 1),
]
FIRST = [(1, 0, 0), (3, 0, 0), (0, 1, 0)]
SECOND = [(0, 1, 1), (1, 0, 1), (3, 0, 1), (0, 0, 1)]
THIRD = STEPS[:8]
NEAR = [(1, 0), (3, 0), (0, 1)]
MAIN = 1
LOADS = 4


def kernel(
    g_hbm, m_hbm, w_hbm, nw, nm, g, m, w, out, part, group, pair, final,
    load, send, recv, p_send, p_recv, t_send, t_recv, ready,
):
    col, row = lax.axis_index("col"), lax.axis_index("row")
    x, y, c = col // (NY * NC), (col // NC) % NY, col % NC
    h, z = row // NZ, row % NZ

    def place(a, b, k):
        return ((x + a) % NX) * (NY * NC) + ((y + b) % NY) * NC + k

    def partner(step):
        a, b, k = step
        return place(a, b, (c + k) % NC)

    def columns(p):
        return pl.ds(pl.multiple_of(p * COLS, 128), COLS)

    def rows_of(p):
        return pl.ds(pl.multiple_of(p * ROWS, ROWS), ROWS)

    def wait_for(ref, sem):
        pltpu.make_async_copy(ref, ref, sem).wait()

    order = [partner(s) for s in STEPS] + [col]
    first, second, third = ([STEPS.index(s) for s in part_of] for part_of in (FIRST, SECOND, THIRD))
    later = second + third + [PEERS - 1]

    for i in first:
        pltpu.make_async_copy(w_hbm.at[:, columns(order[i])], w.at[order[i]], load.at[0]).start()

    near = [{"col": place(a, b, c)} for a, b in NEAR]
    other = {"col": place(0, 0, 1 - c)}
    outside = [
        {"row": (1 - h) * NZ + z, "col": partner((0, 1, 0))},
        {"row": h * NZ + z + 1 - 2 * (z % 2), "col": col},
        {"row": h * NZ + NZ - 1 - z, "col": col},
    ]

    asks = [h == 0, z % 2 == 0, z < NZ // 2]
    asked = h + z % 2 + z // (NZ // 2)

    barrier = pltpu.get_barrier_semaphore()
    for ids in near:
        pl.semaphore_signal(barrier, inc=1, device_id=ids, device_id_type=MESH)

    @pl.when(c == MAIN)
    def _():
        pl.semaphore_signal(barrier, inc=1, device_id=other, device_id_type=MESH)

    for ask, ids in zip(asks, outside):

        @pl.when((c != MAIN) & ask)
        def _():
            pl.semaphore_signal(barrier, inc=1, device_id=ids, device_id_type=MESH)

    def load_rows(src, dst, k):
        size = ROWS // LOADS
        for j in range(LOADS):
            rows = pl.ds(j * size, size)
            pltpu.make_async_copy(src.at[rows], dst.at[rows], load.at[k]).start()

    load_rows(g_hbm, g, 1)

    def block_copy(src, dst, k, i):
        return pltpu.make_async_remote_copy(
            src_ref=src.at[order[i]], dst_ref=dst.at[rows_of(col)],
            send_sem=send.at[k], recv_sem=recv.at[k], device_id={"col": order[i]}, device_id_type=MESH,
        )

    wait_for(w.at[pl.ds(0, len(first))], load.at[0])

    @pl.when(c == MAIN)
    def _():
        pl.semaphore_wait(barrier, len(NEAR))

    @pl.when(c != MAIN)
    def _():
        pl.semaphore_wait(barrier, len(NEAR) + 1 + asked)
        pl.semaphore_signal(ready.at[0], inc=1, device_id=other, device_id_type=MESH)

    for i in first:
        block_copy(w, nw, 0, i).start()
    for i in later:
        pltpu.make_async_copy(w_hbm.at[:, columns(order[i])], w.at[order[i]], load.at[2]).start()
    load_rows(m_hbm, m, 3)

    @pl.when(c == MAIN)
    def _():
        pl.semaphore_wait(ready.at[0], 1)
        for ids in near:
            pl.semaphore_signal(ready.at[1], inc=1, device_id=ids, device_id_type=MESH)
        pl.semaphore_wait(ready.at[1], len(NEAR))
        for ids in near:
            pl.semaphore_signal(ready.at[2], inc=1, device_id=ids, device_id_type=MESH)

    for j, (ask, ids) in enumerate(zip(asks, outside)):

        @pl.when((c != MAIN) & jnp.logical_not(ask))
        def _():
            pl.semaphore_signal(ready.at[3 + j], inc=1, device_id=ids, device_id_type=MESH)

    wait_for(g, load.at[1])
    acc = jnp.zeros((8, COLS), jnp.float32)
    for i in range(PEERS):
        for r in range(0, ROWS, 8):
            v = g[r : r + 8, i * COLS : (i + 1) * COLS]
            acc = acc + v * v
    acc = jnp.sum(acc, axis=0, keepdims=True)
    own = acc[:, 0:128]
    for j in range(128, COLS, 128):
        own = own + acc[:, j : j + 128]
    part[0] = own
    group[col] = own

    @pl.when(c == MAIN)
    def _():
        pl.semaphore_wait(ready.at[2], len(NEAR))
        pl.semaphore_signal(ready.at[1], inc=1, device_id=other, device_id_type=MESH)

    @pl.when(c != MAIN)
    def _():
        pl.semaphore_wait(ready.at[1], 1)

    for i in range(PEERS - 1):
        pltpu.make_async_remote_copy(
            src_ref=part.at[0], dst_ref=group.at[col], send_sem=send.at[2], recv_sem=recv.at[2],
            device_id={"col": order[i]}, device_id_type=MESH,
        ).start()
    wait_for(group.at[pl.ds(0, PEERS - 1)], send.at[2])
    wait_for(w.at[pl.ds(0, len(later))], load.at[2])

    for i in second:
        block_copy(w, nw, 0, i).start()

    wait_for(group.at[pl.ds(0, PEERS - 1)], recv.at[2])
    for i in third:
        block_copy(w, nw, 0, i).start()

    total = group[0]
    for j in range(1, PEERS):
        total = total + group[j]

    told = pltpu.make_async_remote_copy(
        src_ref=part.at[4], dst_ref=final.at[0], send_sem=t_send, recv_sem=t_recv,
        device_id=other, device_id_type=MESH,
    )

    @pl.when(c != MAIN)
    def _():
        value = total
        for j, ids in enumerate(outside):
            part[1 + j] = value

            @pl.when(asks[j])
            def _():
                pl.semaphore_wait(ready.at[3 + j], 1)

            copy = pltpu.make_async_remote_copy(
                src_ref=part.at[1 + j], dst_ref=pair.at[j], send_sem=p_send.at[j], recv_sem=p_recv.at[j],
                device_id=ids, device_id_type=MESH,
            )
            copy.start()
            copy.wait()
            value = value + pair[j]
        part[4] = value
        final[0] = value
        told.start()
        told.wait_send()

    @pl.when(c == MAIN)
    def _():
        told.wait_recv()

    total = jnp.sum(final[0], axis=1, keepdims=True)
    factor = jnp.minimum(jnp.float32(1.0), jnp.float32(LIMIT) / (jnp.sqrt(total) + jnp.float32(1e-06)))

    wait_for(m, load.at[3])
    for i, p in enumerate(order):
        out[p] = jnp.float32(0.9) * m[:, columns(p)] + factor * g[:, columns(p)]
        if i:
            block_copy(out, nm, 1, i - 1).start()

    nm[rows_of(col)] = out[col]
    nw[rows_of(col)] = w[col]
    for k, ref in enumerate((nw, nm)):
        wait_for(ref.at[pl.ds(0, (PEERS - 1) * ROWS)], recv.at[k])
    for k, ref in enumerate((nw, nm)):
        wait_for(ref.at[pl.ds(0, (PEERS - 1) * ROWS)], send.at[k])


def store(w, nm, nw_hbm, nm_hbm, nw, sem):
    size = w.shape[0] // PIECES

    def piece(src, dst, k, i):
        rows = pl.ds(i * size, size)
        return pltpu.make_async_copy(src.at[rows], dst.at[rows], sem.at[k])

    for i in range(PIECES):
        piece(nm, nm_hbm, 0, i).start()
    for i in range(PIECES):
        rows = pl.ds(i * size, size)
        nw[rows] = w[rows] - jnp.float32(0.1) * nm[rows]
        if i:
            piece(nw, nw_hbm, 1, i - 1).start()
    piece(nw, nw_hbm, 1, PIECES - 1).start()
    pltpu.make_async_copy(nm, nm_hbm, sem.at[0]).wait()
    pltpu.make_async_copy(nw, nw_hbm, sem.at[1]).wait()


def body(grad, momentum, weight):
    f32 = jnp.float32
    dma = pltpu.SemaphoreType.DMA
    blocks = pltpu.VMEM((PEERS, ROWS, COLS), f32)
    whole = pltpu.VMEM((ROWS, PEERS * COLS), f32)
    outs = [jax.ShapeDtypeStruct((PEERS * ROWS, COLS), f32)] * 2
    landed = pl.pallas_call(
        kernel,
        out_shape=outs,
        in_specs=[pl.BlockSpec(memory_space=pl.ANY)] * 3,
        out_specs=[pl.BlockSpec(memory_space=pltpu.VMEM)] * 2,
        scratch_shapes=[
            whole, whole, blocks, blocks,
            pltpu.VMEM((5, 1, 128), f32),
            pltpu.VMEM((PEERS, 1, 128), f32),
            pltpu.VMEM((3, 1, 128), f32),
            pltpu.VMEM((1, 1, 128), f32),
            dma((4,)), dma((3,)), dma((3,)), dma((3,)), dma((3,)), dma, dma,
            pltpu.SemaphoreType.REGULAR((6,)),
        ],
        compiler_params=pltpu.CompilerParams(
            collective_id=0, has_side_effects=True, vmem_limit_bytes=45 * 2**20
        ),
    )(grad, momentum, weight)
    return pl.pallas_call(
        store,
        out_shape=outs,
        in_specs=[pl.BlockSpec(memory_space=pltpu.VMEM)] * 2,
        out_specs=[pl.BlockSpec(memory_space=pl.ANY)] * 2,
        scratch_shapes=[pltpu.VMEM((PEERS * ROWS, COLS), f32), dma((2,))],
        compiler_params=pltpu.CompilerParams(vmem_limit_bytes=8 * 2**20),
    )(*landed)


def solution(mesh):
    return jax.shard_map(
        body,
        mesh=mesh,
        in_specs=(P(("row", "col"), None),) * 3,
        out_specs=(P("row", "col"),) * 2,
        check_vma=False,
    )
```

```python
import math

import jax
import jax.numpy as jnp
from jax import lax
from jax.experimental import pallas as pl
from jax.experimental.pallas import tpu as pltpu
from jax.sharding import PartitionSpec as P

D = 8192
FF = 14336
MESH = pl.DeviceIdType.MESH
LIMIT = math.sqrt(D * FF)

NX, NY, NC = 4, 2, 2
NZ = 4
PEERS = NX * NY * NC
ROWS, COLS = 64, 896
PIECES = 16

STEPS = [
    (2, 1, 1), (2, 1, 0), (1, 1, 1), (1, 1, 0), (2, 0, 1), (2, 0, 0), (3, 1, 1), (3, 1, 0),
    (0, 1, 1), (0, 1, 0), (1, 0, 1), (1, 0, 0), (3, 0, 1), (3, 0, 0), (0, 0, 1),
]
FIRST = [(1, 0, 0), (3, 0, 0), (0, 1, 0)]
SECOND = [(0, 1, 1), (1, 0, 1), (3, 0, 1), (0, 0, 1)]
THIRD = STEPS[:8]
NEAR = [(1, 0), (3, 0), (0, 1)]
MAIN = 1
LOADS = 4


def kernel(
    g_hbm, m_hbm, w_hbm, nw, nm, g, m, w, out, part, group, pair, final,
    load, send, recv, p_send, p_recv, t_send, t_recv, ready,
):
    col, row = lax.axis_index("col"), lax.axis_index("row")
    x, y, c = col // (NY * NC), (col // NC) % NY, col % NC
    h, z = row // NZ, row % NZ

    def place(a, b, k):
        return ((x + a) % NX) * (NY * NC) + ((y + b) % NY) * NC + k

    def partner(step):
        a, b, k = step
        return place(a, b, (c + k) % NC)

    def columns(p):
        return pl.ds(pl.multiple_of(p * COLS, 128), COLS)

    def rows_of(p):
        return pl.ds(pl.multiple_of(p * ROWS, ROWS), ROWS)

    def wait_for(ref, sem):
        pltpu.make_async_copy(ref, ref, sem).wait()

    order = [partner(s) for s in STEPS] + [col]
    first, second, third = ([STEPS.index(s) for s in part_of] for part_of in (FIRST, SECOND, THIRD))
    later = second + third + [PEERS - 1]

    for i in first:
        pltpu.make_async_copy(w_hbm.at[:, columns(order[i])], w.at[order[i]], load.at[0]).start()

    near = [{"col": place(a, b, c)} for a, b in NEAR]
    other = {"col": place(0, 0, 1 - c)}
    outside = [
        {"row": (1 - h) * NZ + z, "col": partner((0, 1, 0))},
        {"row": h * NZ + z + 1 - 2 * (z % 2), "col": col},
        {"row": h * NZ + NZ - 1 - z, "col": col},
    ]

    asks = [h == 0, z % 2 == 0, z < NZ // 2]
    asked = h + z % 2 + z // (NZ // 2)

    barrier = pltpu.get_barrier_semaphore()
    for ids in near:
        pl.semaphore_signal(barrier, inc=1, device_id=ids, device_id_type=MESH)

    @pl.when(c == MAIN)
    def _():
        pl.semaphore_signal(barrier, inc=1, device_id=other, device_id_type=MESH)

    for ask, ids in zip(asks, outside):

        @pl.when((c != MAIN) & ask)
        def _():
            pl.semaphore_signal(barrier, inc=1, device_id=ids, device_id_type=MESH)

    def load_rows(src, dst, k):
        size = ROWS // LOADS
        for j in range(LOADS):
            rows = pl.ds(j * size, size)
            pltpu.make_async_copy(src.at[rows], dst.at[rows], load.at[k]).start()

    load_rows(g_hbm, g, 1)

    def block_copy(src, dst, k, i):
        return pltpu.make_async_remote_copy(
            src_ref=src.at[order[i]], dst_ref=dst.at[rows_of(col)],
            send_sem=send.at[k], recv_sem=recv.at[k], device_id={"col": order[i]}, device_id_type=MESH,
        )

    wait_for(w.at[pl.ds(0, len(first))], load.at[0])

    @pl.when(c == MAIN)
    def _():
        pl.semaphore_wait(barrier, len(NEAR))

    @pl.when(c != MAIN)
    def _():
        pl.semaphore_wait(barrier, len(NEAR) + 1 + asked)
        pl.semaphore_signal(ready.at[0], inc=1, device_id=other, device_id_type=MESH)

    for i in first:
        block_copy(w, nw, 0, i).start()
    for i in later:
        pltpu.make_async_copy(w_hbm.at[:, columns(order[i])], w.at[order[i]], load.at[2]).start()
    load_rows(m_hbm, m, 3)

    @pl.when(c == MAIN)
    def _():
        pl.semaphore_wait(ready.at[0], 1)
        for ids in near:
            pl.semaphore_signal(ready.at[1], inc=1, device_id=ids, device_id_type=MESH)
        pl.semaphore_wait(ready.at[1], len(NEAR))
        for ids in near:
            pl.semaphore_signal(ready.at[2], inc=1, device_id=ids, device_id_type=MESH)

    for j, (ask, ids) in enumerate(zip(asks, outside)):

        @pl.when((c != MAIN) & jnp.logical_not(ask))
        def _():
            pl.semaphore_signal(ready.at[3 + j], inc=1, device_id=ids, device_id_type=MESH)

    wait_for(g, load.at[1])
    acc = jnp.zeros((8, COLS), jnp.float32)
    for i in range(PEERS):
        for r in range(0, ROWS, 8):
            v = g[r : r + 8, i * COLS : (i + 1) * COLS]
            acc = acc + v * v
    acc = jnp.sum(acc, axis=0, keepdims=True)
    own = acc[:, 0:128]
    for j in range(128, COLS, 128):
        own = own + acc[:, j : j + 128]
    part[0] = own
    group[col] = own

    @pl.when(c == MAIN)
    def _():
        pl.semaphore_wait(ready.at[2], len(NEAR))
        pl.semaphore_signal(ready.at[1], inc=1, device_id=other, device_id_type=MESH)

    @pl.when(c != MAIN)
    def _():
        pl.semaphore_wait(ready.at[1], 1)

    for i in range(PEERS - 1):
        pltpu.make_async_remote_copy(
            src_ref=part.at[0], dst_ref=group.at[col], send_sem=send.at[2], recv_sem=recv.at[2],
            device_id={"col": order[i]}, device_id_type=MESH,
        ).start()
    wait_for(group.at[pl.ds(0, PEERS - 1)], send.at[2])
    wait_for(w.at[pl.ds(0, len(later))], load.at[2])

    for i in second:
        block_copy(w, nw, 0, i).start()

    wait_for(group.at[pl.ds(0, PEERS - 1)], recv.at[2])
    for i in third:
        block_copy(w, nw, 0, i).start()

    total = group[0]
    for j in range(1, PEERS):
        total = total + group[j]

    told = pltpu.make_async_remote_copy(
        src_ref=part.at[4], dst_ref=final.at[0], send_sem=t_send, recv_sem=t_recv,
        device_id=other, device_id_type=MESH,
    )

    @pl.when(c != MAIN)
    def _():
        value = total
        for j, ids in enumerate(outside):
            part[1 + j] = value

            @pl.when(asks[j])
            def _():
                pl.semaphore_wait(ready.at[3 + j], 1)

            copy = pltpu.make_async_remote_copy(
                src_ref=part.at[1 + j], dst_ref=pair.at[j], send_sem=p_send.at[j], recv_sem=p_recv.at[j],
                device_id=ids, device_id_type=MESH,
            )
            copy.start()
            copy.wait()
            value = value + pair[j]
        part[4] = value
        final[0] = value
        told.start()
        told.wait_send()

    @pl.when(c == MAIN)
    def _():
        told.wait_recv()

    total = jnp.sum(final[0], axis=1, keepdims=True)
    factor = jnp.minimum(jnp.float32(1.0), jnp.float32(LIMIT) / (jnp.sqrt(total) + jnp.float32(1e-06)))

    wait_for(m, load.at[3])
    for i, p in enumerate(order):
        out[p] = jnp.float32(0.9) * m[:, columns(p)] + factor * g[:, columns(p)]
        if i:
            block_copy(out, nm, 1, i - 1).start()

    nm[rows_of(col)] = out[col]
    nw[rows_of(col)] = w[col]
    for k, ref in enumerate((nw, nm)):
        wait_for(ref.at[pl.ds(0, (PEERS - 1) * ROWS)], recv.at[k])
    for k, ref in enumerate((nw, nm)):
        wait_for(ref.at[pl.ds(0, (PEERS - 1) * ROWS)], send.at[k])


def store(w, nm, nw_hbm, nm_hbm, nw, sem):
    size = w.shape[0] // PIECES

    def piece(src, dst, k, i):
        rows = pl.ds(i * size, size)
        return pltpu.make_async_copy(src.at[rows], dst.at[rows], sem.at[k])

    for i in range(PIECES):
        piece(nm, nm_hbm, 0, i).start()
    for i in range(PIECES):
        rows = pl.ds(i * size, size)
        nw[rows] = w[rows] - jnp.float32(0.1) * nm[rows]
        if i:
            piece(nw, nw_hbm, 1, i - 1).start()
    piece(nw, nw_hbm, 1, PIECES - 1).start()
    pltpu.make_async_copy(nm, nm_hbm, sem.at[0]).wait()
    pltpu.make_async_copy(nw, nw_hbm, sem.at[1]).wait()


def body(grad, momentum, weight):
    f32 = jnp.float32
    dma = pltpu.SemaphoreType.DMA
    blocks = pltpu.VMEM((PEERS, ROWS, COLS), f32)
    whole = pltpu.VMEM((ROWS, PEERS * COLS), f32)
    outs = [jax.ShapeDtypeStruct((PEERS * ROWS, COLS), f32)] * 2
    landed = pl.pallas_call(
        kernel,
        out_shape=outs,
        in_specs=[pl.BlockSpec(memory_space=pl.ANY)] * 3,
        out_specs=[pl.BlockSpec(memory_space=pltpu.VMEM)] * 2,
        scratch_shapes=[
            whole, whole, blocks, blocks,
            pltpu.VMEM((5, 1, 128), f32),
            pltpu.VMEM((PEERS, 1, 128), f32),
            pltpu.VMEM((3, 1, 128), f32),
            pltpu.VMEM((1, 1, 128), f32),
            dma((4,)), dma((3,)), dma((3,)), dma((3,)), dma((3,)), dma, dma,
            pltpu.SemaphoreType.REGULAR((6,)),
        ],
        compiler_params=pltpu.CompilerParams(
            collective_id=0, has_side_effects=True, vmem_limit_bytes=45 * 2**20
        ),
    )(grad, momentum, weight)
    return pl.pallas_call(
        store,
        out_shape=outs,
        in_specs=[pl.BlockSpec(memory_space=pltpu.VMEM)] * 2,
        out_specs=[pl.BlockSpec(memory_space=pl.ANY)] * 2,
        scratch_shapes=[pltpu.VMEM((PEERS * ROWS, COLS), f32), dma((2,))],
        compiler_params=pltpu.CompilerParams(vmem_limit_bytes=8 * 2**20),
    )(*landed)


def solution(mesh):
    return jax.shard_map(
        body,
        mesh=mesh,
        in_specs=(P(("row", "col"), None),) * 3,
        out_specs=(P("row", "col"),) * 2,
        check_vma=False,
    )
```
